32 devices in a mesh: dp: 1 (over z), ing: 4 (over y), grp: 8 (over x, core).
Axes of the slice: x: 4, y: 4, z: 1, core: 2. Of those that a mesh axis runs over, the one named last changes fastest.
The devices are a block of a 4x4x8 slice.
Arguments:
- x_first: bfloat16 [49152, 1024], P(('dp', 'grp', 'ing'))
- ids_first: int32 [49152, 8], P(('dp', 'grp', 'ing'))
- gates_first: float32 [49152, 8], P(('dp', 'grp', 'ing'))
- x_second: bfloat16 [49152, 1024], P(('dp', 'grp', 'ing'))
- ids_second: int32 [49152, 8], P(('dp', 'grp', 'ing'))
- gates_second: float32 [49152, 8], P(('dp', 'grp', 'ing'))
- w_one: bfloat16 [32, 1024, 512], P(('grp', 'ing'))
- w_three: bfloat16 [32, 1024, 512], P(('grp', 'ing'))
- w_two: bfloat16 [32, 512, 1024], P(('grp', 'ing'))
Outputs:
- output 1: bfloat16 [49152, 1024], P(('dp', 'grp', 'ing'))
- output 2: bfloat16 [49152, 1024], P(('dp', 'grp', 'ing'))
All inputs are finite; a program needn't handle non-finite values.
Results may differ from the reference program's by a relative error of at most 0.0087765.
Values are sent between devices in bfloat16 or wider.
A program may use at most 768 MiB of HBM per device.

```python
import jax
import jax.numpy as jnp
from jax import lax

HIDDEN = 1024
EXPERT_FF = 512
EXPERTS = 32
TOP_K = 8
GROUPS = 8
INNER_DEV = 4
TOKENS = 1536

SOURCES = GROUPS * INNER_DEV
ROWS_ALL = SOURCES * TOKENS
PER_GROUP = EXPERTS // GROUPS
LIMIT_M = min(TOP_K, GROUPS // 2)
PER_SLOT = TOP_K // LIMIT_M
GROUP_STEP = GROUPS // LIMIT_M
CAP_EXPERT = LIMIT_M * ((TOKENS * PER_SLOT + EXPERTS - 1) // EXPERTS)
EXPERT_ROWS = SOURCES * CAP_EXPERT


def route_source(tok_perm, grp_perm, loc_perm, offset):
    position = tok_perm[:, None, None]
    slot_q = jnp.arange(LIMIT_M)[None, :, None]
    slot_u = jnp.arange(PER_SLOT)[None, None, :]
    grp_id = grp_perm[(position + slot_q * GROUP_STEP) % GROUPS]
    residue = ((position // GROUPS) * PER_SLOT + slot_u + offset) % PER_GROUP
    local_id = loc_perm[grp_id, residue]
    return (grp_id * PER_GROUP + local_id).reshape(TOKENS, TOP_K)


def draw_routing(key_in):
    key_tok, key_grp, key_loc, key_off = jax.random.split(key_in, 4)
    tok_perm = jax.vmap(lambda sub_key: jax.random.permutation(sub_key, TOKENS))(jax.random.split(key_tok, SOURCES))
    grp_perm = jax.vmap(lambda sub_key: jax.random.permutation(sub_key, GROUPS))(jax.random.split(key_grp, SOURCES))
    loc_keys = jax.random.split(key_loc, SOURCES * GROUPS)
    loc_perm = jax.vmap(lambda sub_key: jax.random.permutation(sub_key, PER_GROUP))(loc_keys).reshape(SOURCES, GROUPS, PER_GROUP)
    offset = jax.random.randint(key_off, (SOURCES,), 0, PER_GROUP)
    expert_ids = jax.vmap(route_source)(tok_perm, grp_perm, loc_perm, offset)
    return expert_ids.reshape(ROWS_ALL, TOP_K).astype(jnp.int32)


def draw_gates(key_in):
    return jax.random.uniform(key_in, (ROWS_ALL, TOP_K), jnp.float32, 0.2, 1.8) / TOP_K


def draw_weights(key_in, fan_in, fan_out):
    expert_keys = jax.random.split(key_in, EXPERTS)
    scale_in = fan_in ** -0.5
    return lax.map(lambda sub_key: (jax.random.normal(sub_key, (fan_in, fan_out), jnp.float32) * scale_in).astype(jnp.bfloat16), expert_keys)


def setup_inputs(seed: int = 0, part: int = 0) -> dict:
    root_key = jax.random.key(seed)
    key_data, key_weight = jax.random.split(root_key)
    key_part = jax.random.fold_in(key_data, part)
    data_keys = jax.random.split(key_part, 6)
    weight_keys = jax.random.split(key_weight, 3)
    return {
        'x_first': jax.random.normal(data_keys[0], (ROWS_ALL, HIDDEN), jnp.float32).astype(jnp.bfloat16),
        'ids_first': draw_routing(data_keys[1]),
        'gates_first': draw_gates(data_keys[2]),
        'x_second': jax.random.normal(data_keys[3], (ROWS_ALL, HIDDEN), jnp.float32).astype(jnp.bfloat16),
        'ids_second': draw_routing(data_keys[4]),
        'gates_second': draw_gates(data_keys[5]),
        'w_one': draw_weights(weight_keys[0], HIDDEN, EXPERT_FF),
        'w_three': draw_weights(weight_keys[1], HIDDEN, EXPERT_FF),
        'w_two': draw_weights(weight_keys[2], EXPERT_FF, HIDDEN),
    }


def moe_layer(tokens_in, expert_ids, gate_vals, w_one, w_three, w_two):
    w_stack = (w_one.reshape(GROUPS, PER_GROUP, HIDDEN, EXPERT_FF),
               w_three.reshape(GROUPS, PER_GROUP, HIDDEN, EXPERT_FF),
               w_two.reshape(GROUPS, PER_GROUP, EXPERT_FF, HIDDEN))
    row_range = jnp.arange(EXPERT_ROWS)

    def expert_step(acc_sum, expert_in):
        e_one, e_three, e_two, expert = expert_in
        expert_hit = expert_ids == expert
        member = jnp.any(expert_hit, axis=1)
        gate_col = jnp.sum(jnp.where(expert_hit, gate_vals, 0.0), axis=1)
        row_count = jnp.sum(member.astype(jnp.int32))
        row_ids = jnp.nonzero(member, size=EXPERT_ROWS, fill_value=0)[0]
        row_gate = jnp.where(row_range < row_count, gate_col[row_ids], 0.0)
        picked = tokens_in[row_ids]
        act_a = jnp.dot(picked, e_one, preferred_element_type=jnp.float32)
        act_b = jnp.dot(picked, e_three, preferred_element_type=jnp.float32)
        hidden_act = (jax.nn.silu(act_a) * act_b).astype(jnp.bfloat16)
        expert_out = jnp.dot(hidden_act, e_two, preferred_element_type=jnp.float32)
        scaled = (expert_out * row_gate[:, None]).astype(jnp.bfloat16)
        return acc_sum.at[row_ids].add(scaled.astype(jnp.float32)), None

    def group_step(y_acc, group_in):
        g_one, g_three, g_two, group_id = group_in
        expert_list = group_id * PER_GROUP + jnp.arange(PER_GROUP)
        zero_acc = jnp.zeros((ROWS_ALL, HIDDEN), jnp.float32)
        group_acc, _ = lax.scan(expert_step, zero_acc, (g_one, g_three, g_two, expert_list))
        return y_acc + group_acc.astype(jnp.bfloat16).astype(jnp.float32), None

    y_init = jnp.zeros((ROWS_ALL, HIDDEN), jnp.float32)
    y_acc, _ = lax.scan(group_step, y_init, w_stack + (jnp.arange(GROUPS),))
    return y_acc.astype(jnp.bfloat16)


def reference(x_first, ids_first, gates_first, x_second, ids_second, gates_second, w_one, w_three, w_two):
    y_first = moe_layer(x_first, ids_first, gates_first, w_one, w_three, w_two)
    y_second = moe_layer(x_second, ids_second, gates_second, w_one, w_three, w_two)
    return (y_first, y_second)
```

```python
import functools

import jax
import jax.numpy as jnp
from jax import lax
from jax.experimental import pallas as pl
from jax.experimental.pallas import tpu as pltpu
from jax.sharding import PartitionSpec as P

MESH = pl.DeviceIdType.MESH
AHEAD = 8
RING = 4
ORDER = [(0, 0), (0, 1), (0, 3), (0, 2), (1, 0), (3, 0), (1, 1), (1, 3), (3, 1), (3, 3), (1, 2), (3, 2), (2, 0), (2, 1), (2, 3), (2, 2)]
GROUP_DX = [0, 0, 1, 1, 3, 3, 2, 2]
UNIT_STEP = {1: 3, 2: 6, 3: 8, 4: 9, 5: 11, 6: 13, 7: 15, 8: 15, 9: 17, 10: 18, 11: 20, 12: 22, 13: 25, 14: 27, 15: 31}


def link_sends():
    lists = []
    for d in (1, -1):
        kf, kg = (0, 2) if d > 0 else (1, 3)
        sends = [(0, 0, k) for k in (0, 1, 2, 3)] + [(-d, 0, kf), (-d, 0, kg)]
        sends += [(0, b, k) for b in (1, -1, 2) for k in (2, 3)] + [(-d, b, kg) for b in (1, -1, 2)]
        lists.append([(a % RING, b % RING, k) for a, b, k in sends])
    for d in (1, -1):
        kf, kg = (0, 2) if d > 0 else (1, 3)
        sends = [(0, 0, k) for k in (2, 3, 0, 1)] + [(0, -d, kg), (0, -d, kf)]
        sends += [(a, 0, k) for a in (1, -1) for k in (0, 1)] + [(a, -d, kf) for a in (1, -1)]
        sends += [(2, 0, 0), (2, 0, 1), (2, -d, kf)]
        lists.append([(a % RING, b % RING, k) for a, b, k in sends])
    return lists


STEP_OF_LINK = [(1, 0), (-1, 0), (0, 1), (0, -1)]


def make_plan():
    sends = link_sends()
    units = len(sends[0])
    shifted = lambda link, item: ((item[0] - STEP_OF_LINK[link][0]) % RING, (item[1] - STEP_OF_LINK[link][1]) % RING, item[2])
    have = {(0, 0, k) for k in range(4)}
    nxt = [0] * 4
    plan = {}
    done = set()
    for unit in range(units + 1):
        arrivals = [] if unit == 0 else [shifted(link, sends[link][unit - 1]) for link in range(4)]
        assert not have & set(arrivals)
        have |= set(arrivals)
        issued = []
        moved = True
        while moved:
            moved = False
            for link in range(4):
                if nxt[link] < units and sends[link][nxt[link]] in have:
                    issued.append((link, nxt[link], sends[link][nxt[link]], shifted(link, sends[link][nxt[link]])))
                    nxt[link] += 1
                    moved = True
        complete = [p for p in ORDER if p not in done and all((*p, k) in have for k in range(4))]
        done |= set(complete)
        plan[unit] = (arrivals, issued, complete)
    assert len(have) == 4 * RING * RING and nxt == [units] * 4
    return plan, units


def pick(index, values):
    out = jnp.int32(values[0])
    for i, v in enumerate(values[1:], 1):
        out = jnp.where(index == i, jnp.int32(v), out)
    return out


def kernel(cap, x_first, x_second, ids_ref, gates_ref, wown, y_first, y_second, wall, zh,
           xv, yacc, wv, xg, gb, zst, zc, slotrow, gaterow, slotcol,
           recv_sem, send_sem, d2d_recv, d2d_send, w_sem, x_sem, z_sem, zl_sem, y_sem):
    grp, y = lax.axis_index('grp'), lax.axis_index('ing')
    x, c = grp // 2, grp % 2
    tokens = xv.shape[1]
    experts = slotrow.shape[1]
    per_group = RING
    plan, units = make_plan()
    npos = RING * RING

    def expert(dx, dy, core):
        return (((x + dx) % RING) * 2 + core) * per_group + (y + dy) % RING

    def neighbour(link):
        sx, sy = STEP_OF_LINK[link]
        return {'grp': ((x + sx) % RING) * 2 + c, 'ing': (y + sy) % RING}

    partner = {'grp': x * 2 + (1 - c), 'ing': y}

    barrier = pltpu.get_barrier_semaphore()
    for dev in [neighbour(link) for link in range(4)] + [partner]:
        pl.semaphore_signal(barrier, inc=1, device_id=dev, device_id_type=MESH)
    pl.semaphore_wait(barrier, 5)

    def quarter_copy(link, slot, item, target):
        dx, dy, k = item
        e = expert(dx, dy, c)
        src = wown.at[:, k] if (dx, dy) == (0, 0) else wall.at[e, :, k]
        return pltpu.make_async_remote_copy(
            src_ref=src, dst_ref=wall.at[e, :, k], send_sem=send_sem.at[link * units + slot],
            recv_sem=recv_sem.at[(target[0] * RING + target[1]) * 4 + k], device_id=neighbour(link), device_id_type=MESH)

    def d2d_copy(pos):
        j = ORDER.index(pos)
        e = expert(*pos, c)
        src = wown if j == 0 else wall.at[e]
        return pltpu.make_async_remote_copy(
            src_ref=src, dst_ref=wall.at[e], send_sem=d2d_send.at[j], recv_sem=d2d_recv.at[j],
            device_id=partner, device_id_type=MESH)

    def act(unit):
        arrivals, issued, complete = plan[unit]
        for dx, dy, k in arrivals:
            ref = wall.at[expert(dx, dy, c), :, k]
            pltpu.make_async_remote_copy(
                src_ref=ref, dst_ref=ref, send_sem=send_sem.at[0], recv_sem=recv_sem.at[(dx * RING + dy) * 4 + k],
                device_id=partner, device_id_type=MESH).wait_recv()
        for link, slot, item, target in issued:
            quarter_copy(link, slot, item, target).start()
        for pos in complete:
            d2d_copy(pos).start()

    act(0)
    x_copies = [pltpu.make_async_copy(src, xv.at[m], x_sem.at[m]) for m, src in enumerate((x_first, x_second))]
    for copy in x_copies:
        copy.start()
    pltpu.make_async_copy(wown, wv.at[0], w_sem.at[0]).start()

    lane_block = 128
    upper = (lax.broadcasted_iota(jnp.int32, (lane_block, lane_block), 0)
             <= lax.broadcasted_iota(jnp.int32, (lane_block, lane_block), 1)).astype(jnp.bfloat16)
    for m in range(2):
        e_iota = lax.broadcasted_iota(jnp.int32, (experts, lane_block), 0)
        carry = jnp.zeros((experts, 1), jnp.float32)
        for b in range(tokens // lane_block):
            cols = pl.ds(b * lane_block, lane_block)
            mem = jnp.zeros((experts, lane_block), jnp.float32)
            gat = jnp.zeros((experts, lane_block), jnp.float32)
            for k in range(ids_ref.shape[1]):
                hit = ids_ref[m, k:k + 1, cols] == e_iota
                mem = jnp.where(hit, 1.0, mem)
                gat = jnp.where(hit, gates_ref[m, k:k + 1, cols], gat)
            total = jnp.dot(mem.astype(jnp.bfloat16), upper, preferred_element_type=jnp.float32) + carry
            carry = total[:, lane_block - 1:]
            slot = jnp.where(mem > 0.0, total - 1.0, -1.0)
            slotrow[m, :, cols] = slot.astype(jnp.int32)
            gaterow[m, :, cols] = gat
            full = jnp.concatenate([slot, jnp.full((lane_block - experts, lane_block), -1.0, jnp.float32)], axis=0)
            slotcol[m, cols, :] = full.T.astype(jnp.int32)

    for m in range(2):
        @pl.loop(0, tokens // 128)
        def _(i):
            yacc[m, pl.ds(i * 128, 128), :] = jnp.zeros((128, yacc.shape[2]), jnp.float32)

    for copy in x_copies:
        copy.wait()

    def step_expert(s):
        j = s // 2
        core = (c + s) % 2
        return expert(pick(j, [p[0] for p in ORDER]), pick(j, [p[1] for p in ORDER]), core)

    def gather(s):
        e = step_expert(s)
        ring = s % AHEAD

        @pl.loop(0, 2)
        def _(m):
            mask = slotrow[m, pl.ds(e, 1), :] == lax.broadcasted_iota(jnp.int32, (cap, tokens), 0)
            gb[ring, m] = jnp.sum(jnp.where(mask, gaterow[m, pl.ds(e, 1), :], 0.0), axis=1, keepdims=True)
            xg[ring, m] = jnp.dot(mask.astype(jnp.bfloat16), xv[m], preferred_element_type=jnp.float32).astype(jnp.bfloat16)

    def z_copy(s):
        e = step_expert(s)
        return pltpu.make_async_copy(zst, zh.at[e // per_group, :, pl.ds((e % per_group) * cap, cap), :], z_sem)

    def ffn(s):
        ring = s % AHEAD
        par = s % 2
        width = wv.shape[4]
        depth = 4 * wv.shape[3]
        pltpu.make_async_copy(wall.at[0], wv.at[par], w_sem.at[par]).wait()

        @pl.loop(0, 2)
        def _(m):
            rows = xg[ring, m]
            act_a = jnp.dot(rows, wv[par, 0].reshape(depth, width), preferred_element_type=jnp.float32)
            act_b = jnp.dot(rows, wv[par, 1].reshape(depth, width), preferred_element_type=jnp.float32)
            hid = (jax.nn.silu(act_a) * act_b).astype(jnp.bfloat16)
            gate = gb[ring, m]
            for half in range(2):
                w2 = wv[par, 2, 2 * half:2 * half + 2].reshape(depth // 2, width)
                out = jnp.dot(hid, w2, preferred_element_type=jnp.float32)
                zst[m, :, half * width:(half + 1) * width] = (out * gate).astype(jnp.bfloat16)
        z_copy(s).start()

    def fetch(s):
        par = s % 2
        for j in range(npos):
            @pl.when(s == 2 * j + 1)
            def _():
                ref = wall.at[expert(*ORDER[j], 1 - c)]
                pltpu.make_async_remote_copy(
                    src_ref=ref, dst_ref=ref, send_sem=d2d_send.at[0], recv_sem=d2d_recv.at[j],
                    device_id=partner, device_id_type=MESH).wait_recv()
        pltpu.make_async_copy(wall.at[step_expert(s)], wv.at[par], w_sem.at[par]).start()

    def combine(base, items):
        def load(i):
            t = base + i // 2
            g = ((x + pick(t, GROUP_DX)) % RING) * 2 + (c + t) % 2
            return g, pltpu.make_async_copy(zh.at[g, i % 2], zc.at[i % 2], zl_sem.at[i % 2])

        load(0)[1].start()
        tile = cap

        @pl.loop(0, items)
        def _(i):
            g, copy = load(i)
            copy.wait()

            @pl.when(i + 1 < items)
            def _():
                load(i + 1)[1].start()

            m = i % 2

            @pl.loop(0, tokens // tile)
            def _(r):
                rows = pl.ds(pl.multiple_of(r * tile, tile), tile)
                table = slotcol[m, rows, :]
                lane = lax.broadcasted_iota(jnp.int32, table.shape, 1)
                lane_cap = lax.broadcasted_iota(jnp.int32, (tile, cap), 1)
                parts = []
                for q in range(per_group):
                    col = jnp.sum(jnp.where(lane == g * per_group + q, table, 0), axis=1, keepdims=True)
                    parts.append((col == lane_cap).astype(jnp.bfloat16))
                sel = jnp.concatenate(parts, axis=1)
                part = jnp.dot(sel, zc[m], preferred_element_type=jnp.float32)
                yacc[m, rows, :] += part.astype(jnp.bfloat16).astype(jnp.float32)

    steps = 2 * npos

    @pl.loop(0, steps + AHEAD)
    def _(v):
        s = v - AHEAD

        @pl.when(s >= 0)
        def _():
            ffn(s)

        for unit in range(1, units + 1):
            @pl.when(v == UNIT_STEP[unit])
            def _():
                act(unit)

        @pl.when((s >= 0) & (s + 1 < steps))
        def _():
            fetch(s + 1)

        @pl.when(v < steps)
        def _():
            gather(v)

        @pl.when(s >= 0)
        def _():
            z_copy(s).wait()

        due = (s == 7) | (s == 23) | (s == 31)

        @pl.when(due)
        def _():
            combine(jnp.where(s == 7, 0, jnp.where(s == 23, 2, 6)), jnp.where(s == 23, 8, 4))

    for m, dst in enumerate((y_first, y_second)):
        @pl.loop(0, tokens // 128)
        def _(i):
            rows = pl.ds(pl.multiple_of(i * 128, 128), 128)
            xv[m, rows, :] = yacc[m, rows, :].astype(jnp.bfloat16)
        pltpu.make_async_copy(xv.at[m], dst, y_sem.at[m]).start()
    for m, dst in enumerate((y_first, y_second)):
        pltpu.make_async_copy(xv.at[m], dst, y_sem.at[m]).wait()

    for unit in range(units + 1):
        _, issued, complete = plan[unit]
        for link, slot, item, target in issued:
            quarter_copy(link, slot, item, target).wait_send()
        for pos in complete:
            d2d_copy(pos).wait_send()


def solution(mesh):
    n_grp = mesh.shape['grp']
    n_ing = mesh.shape['ing']
    assert n_grp == 2 * RING and n_ing == RING
    tok_spec = P(('dp', 'grp', 'ing'), None)
    w_spec = P(('grp', 'ing'), None, None)

    def body(x_first, ids_first, gates_first, x_second, ids_second, gates_second, w_one, w_three, w_two):
        tokens, hidden = x_first.shape
        top_k = ids_first.shape[1]
        experts = n_grp * n_ing
        limit_m = min(top_k, n_grp // 2)
        cap = limit_m * (-(-(tokens * (top_k // limit_m)) // experts))
        inner = w_one.shape[2]
        ids = jnp.stack([ids_first.T, ids_second.T])
        gates = jnp.stack([gates_first.T, gates_second.T])
        quarter = hidden // 4
        w2 = w_two[0].reshape(2, inner // 2, 2, hidden // 2).transpose(2, 0, 1, 3).reshape(4, inner // 2, hidden // 2)
        wown = jnp.stack([w_one[0].reshape(4, quarter, inner), w_three[0].reshape(4, quarter, inner), w2])
        bf, f32, i32 = jnp.bfloat16, jnp.float32, jnp.int32
        hbm = pl.BlockSpec(memory_space=pl.ANY)
        vmem = pl.BlockSpec(memory_space=pltpu.VMEM)
        dma = pltpu.SemaphoreType.DMA
        y_shape = jax.ShapeDtypeStruct((tokens, hidden), bf)
        outs = pl.pallas_call(
            functools.partial(kernel, cap),
            out_shape=(y_shape, y_shape,
                       jax.ShapeDtypeStruct((experts,) + wown.shape, bf),
                       jax.ShapeDtypeStruct((n_grp, 2, n_ing * cap, hidden), bf)),
            in_specs=[hbm, hbm, vmem, vmem, hbm],
            out_specs=(hbm,) * 4,
            scratch_shapes=[
                pltpu.VMEM((2, tokens, hidden), bf),
                pltpu.VMEM((2, tokens, hidden), f32),
                pltpu.VMEM((2,) + wown.shape, bf),
                pltpu.VMEM((AHEAD, 2, cap, hidden), bf),
                pltpu.VMEM((AHEAD, 2, cap, 1), f32),
                pltpu.VMEM((2, cap, hidden), bf),
                pltpu.VMEM((2, n_ing * cap, hidden), bf),
                pltpu.VMEM((2, experts, tokens), i32),
                pltpu.VMEM((2, experts, tokens), f32),
                pltpu.VMEM((2, tokens, 128), i32),
                dma((64,)), dma((60,)), dma((16,)), dma((16,)), dma((2,)), dma((2,)), dma(()), dma((2,)), dma((2,)),
            ],
            compiler_params=pltpu.CompilerParams(collective_id=0, has_side_effects=True, vmem_limit_bytes=67043328),
        )(x_first, x_second, ids, gates, wown)
        return outs[0], outs[1]

    return jax.shard_map(body, mesh=mesh, in_specs=(tok_spec,) * 6 + (w_spec,) * 3, out_specs=(tok_spec, tok_spec), check_vma=False)
```

```python
import functools

import jax
import jax.numpy as jnp
from jax import lax
from jax.experimental import pallas as pl
from jax.experimental.pallas import tpu as pltpu
from jax.sharding import PartitionSpec as P

MESH = pl.DeviceIdType.MESH
AHEAD = 20
RING = 4
ORDER = [(0, 0), (0, 1), (0, 3), (1, 0), (3, 0), (0, 2), (1, 1), (1, 3), (1, 2), (3, 1), (3, 3), (3, 2), (2, 0), (2, 1), (2, 3), (2, 2)]
GROUP_DX = [0, 0, 1, 1, 3, 3, 2, 2]
UNIT_STEP = {1: (4, 0), 2: (11, 0), 3: (18, 0), 4: (21, 0), 5: (25, 0), 6: (28, 0), 7: (31, 0), 8: (31, 2), 9: (33, 0), 10: (35, 0),
             11: (37, 2), 12: (39, 0), 13: (43, 1), 14: (43, 2), 15: (47, 0)}


def link_sends():
    lists = []
    for d in (1, -1):
        kf, kg = (0, 2) if d > 0 else (1, 3)
        pair = (2, 3) if d > 0 else (3, 2)
        sends = [(0, 0, k) for k in (0, 1, 2, 3)] + [(0, b, k) for b in (1, -1, 2) for k in pair]
        sends += [(-d, 0, kf), (-d, 0, kg)] + [(-d, b, kg) for b in (1, -1, 2)]
        lists.append([(a % RING, b % RING, k) for a, b, k in sends])
    for d in (1, -1):
        kf, kg = (0, 2) if d > 0 else (1, 3)
        pair = (0, 1) if d > 0 else (1, 0)
        sends = [(0, 0, k) for k in (2, 3, 0, 1)] + [(0, -d, kg), (0, -d, kf)]
        for a in (1, -1, 2):
            sends += [(a, 0, k) for k in pair] + [(a, -d, kf)]
        lists.append([(a % RING, b % RING, k) for a, b, k in sends])
    return lists


STEP_OF_LINK = [(1, 0), (-1, 0), (0, 1), (0, -1)]


def make_plan():
    sends = link_sends()
    units = len(sends[0])
    shifted = lambda link, item: ((item[0] - STEP_OF_LINK[link][0]) % RING, (item[1] - STEP_OF_LINK[link][1]) % RING, item[2])
    have = {(0, 0, k) for k in range(4)}
    nxt = [0] * 4
    plan = {}
    done = set()
    for unit in range(units + 1):
        arrivals = [] if unit == 0 else [shifted(link, sends[link][unit - 1]) for link in range(4)]
        assert not have & set(arrivals)
        have |= set(arrivals)
        issued = []
        moved = True
        while moved:
            moved = False
            for link in range(4):
                if nxt[link] < units and sends[link][nxt[link]] in have:
                    issued.append((link, nxt[link], sends[link][nxt[link]], shifted(link, sends[link][nxt[link]])))
                    nxt[link] += 1
                    moved = True
        complete = [p for p in ORDER if p not in done and all((*p, k) in have for k in range(4))]
        done |= set(complete)
        plan[unit] = (arrivals, issued, complete)
    assert len(have) == 4 * RING * RING and nxt == [units] * 4
    return plan, units


def pick(index, values):
    out = jnp.int32(values[0])
    for i, v in enumerate(values[1:], 1):
        out = jnp.where(index == i, jnp.int32(v), out)
    return out


def kernel(cap, x_first, x_second, ids_ref, gates_ref, wown, y_first, y_second, wall, zh, xh,
           xv, yacc, w13, w2v, xs, xg, gb, zst, zc, slotrow, gaterow, slotcol,
           recv_sem, send_sem, d2d_recv, d2d_send, w_sem, x_sem, xo_sem, xi_sem, z_sem, zl_sem, y_sem):
    grp, y = lax.axis_index('grp'), lax.axis_index('ing')
    x, c = grp // 2, grp % 2
    tokens = xv.shape[1]
    experts = slotrow.shape[1]
    per_group = RING
    width = wown.shape[3]
    plan, units = make_plan()
    npos = RING * RING

    def expert(dx, dy, core):
        return (((x + dx) % RING) * 2 + core) * per_group + (y + dy) % RING

    def neighbour(link):
        sx, sy = STEP_OF_LINK[link]
        return {'grp': ((x + sx) % RING) * 2 + c, 'ing': (y + sy) % RING}

    partner = {'grp': x * 2 + (1 - c), 'ing': y}

    barrier = pltpu.get_barrier_semaphore()
    for dev in [neighbour(link) for link in range(4)] + [partner]:
        pl.semaphore_signal(barrier, inc=1, device_id=dev, device_id_type=MESH)
    pl.semaphore_wait(barrier, 5)

    def quarter_copy(link, slot, item, target):
        dx, dy, k = item
        e = expert(dx, dy, c)
        src = wown.at[:, k] if (dx, dy) == (0, 0) else wall.at[e, :, k]
        return pltpu.make_async_remote_copy(
            src_ref=src, dst_ref=wall.at[e, :, k], send_sem=send_sem.at[link * units + slot],
            recv_sem=recv_sem.at[(target[0] * RING + target[1]) * 4 + k], device_id=neighbour(link), device_id_type=MESH)

    def d2d_copy(pos):
        j = ORDER.index(pos)
        e = expert(*pos, c)
        src = wown if j == 0 else wall.at[e]
        return pltpu.make_async_remote_copy(
            src_ref=src, dst_ref=wall.at[e], send_sem=d2d_send.at[j], recv_sem=d2d_recv.at[j],
            device_id=partner, device_id_type=MESH)

    def act(unit):
        arrivals, issued, complete = plan[unit]
        for dx, dy, k in arrivals:
            ref = wall.at[expert(dx, dy, c), :, k]
            pltpu.make_async_remote_copy(
                src_ref=ref, dst_ref=ref, send_sem=send_sem.at[0], recv_sem=recv_sem.at[(dx * RING + dy) * 4 + k],
                device_id=partner, device_id_type=MESH).wait_recv()
        for link, slot, item, target in issued:
            quarter_copy(link, slot, item, target).start()
        for pos in complete:
            d2d_copy(pos).start()

    act(0)
    x_copies = [pltpu.make_async_copy(src, xv.at[m], x_sem.at[m]) for m, src in enumerate((x_first, x_second))]
    for copy in x_copies:
        copy.start()

    def weight_copies(src, par):
        for half in range(2):
            yield pltpu.make_async_copy(src.at[half], w13.at[par, :, :, pl.ds(half * width, width)], w_sem.at[par * 4 + half])
        for half in range(2):
            yield pltpu.make_async_copy(src.at[2, pl.ds(2 * half, 2)], w2v.at[par, :, :, pl.ds(half * width, width)], w_sem.at[par * 4 + 2 + half])

    for copy in weight_copies(wown, 0):
        copy.start()

    lane_block = 128
    upper = (lax.broadcasted_iota(jnp.int32, (lane_block, lane_block), 0)
             <= lax.broadcasted_iota(jnp.int32, (lane_block, lane_block), 1)).astype(jnp.bfloat16)
    for m in range(2):
        e_iota = lax.broadcasted_iota(jnp.int32, (experts, lane_block), 0)
        carry = jnp.zeros((experts, 1), jnp.float32)
        for b in range(tokens // lane_block):
            cols = pl.ds(b * lane_block, lane_block)
            mem = jnp.zeros((experts, lane_block), jnp.float32)
            gat = jnp.zeros((experts, lane_block), jnp.float32)
            for k in range(ids_ref.shape[1]):
                hit = ids_ref[m, k:k + 1, cols] == e_iota
                mem = jnp.where(hit, 1.0, mem)
                gat = jnp.where(hit, gates_ref[m, k:k + 1, cols], gat)
            total = jnp.dot(mem.astype(jnp.bfloat16), upper, preferred_element_type=jnp.float32) + carry
            carry = total[:, lane_block - 1:]
            slot = jnp.where(mem > 0.0, total - 1.0, -1.0)
            slotrow[m, :, cols] = slot.astype(jnp.int32)
            gaterow[m, :, cols] = gat
            full = jnp.concatenate([slot, jnp.full((lane_block - experts, lane_block), -1.0, jnp.float32)], axis=0)
            slotcol[m, cols, :] = full.T.astype(jnp.int32)

    gb[...] = jnp.zeros_like(gb)
    for m in range(2):
        @pl.loop(0, tokens // 128)
        def _(i):
            yacc[m, pl.ds(i * 128, 128), :] = jnp.zeros((128, yacc.shape[2]), jnp.float32)

    for copy in x_copies:
        copy.wait()

    def step_expert(s):
        j = s // 2
        core = (c + s) % 2
        return expert(pick(j, [p[0] for p in ORDER]), pick(j, [p[1] for p in ORDER]), core)

    def gather(s):
        e = step_expert(s)
        lane = lax.broadcasted_iota(jnp.int32, (cap, gb.shape[2]), 1)
        for m in range(2):
            mask = slotrow[m, pl.ds(e, 1), :] == lax.broadcasted_iota(jnp.int32, (cap, tokens), 0)
            gate = jnp.sum(jnp.where(mask, gaterow[m, pl.ds(e, 1), :], 0.0), axis=1, keepdims=True)
            gb[m] = jnp.where(lane == s, gate, gb[m])
            xs[s % 2, m * cap:(m + 1) * cap, :] = jnp.dot(
                mask.astype(jnp.bfloat16), xv[m], preferred_element_type=jnp.float32).astype(jnp.bfloat16)

    def row_out(s):
        return pltpu.make_async_copy(xs.at[s % 2], xh.at[s], xo_sem.at[s % 2])

    def row_in(s):
        return pltpu.make_async_copy(xh.at[s], xg.at[s % 2], xi_sem.at[s % 2])

    def z_copy(s):
        e = step_expert(s)
        return pltpu.make_async_copy(zst.at[s % 2], zh.at[e // per_group, :, pl.ds((e % per_group) * cap, cap), :], z_sem.at[s % 2])

    def ffn(s):
        par = s % 2
        rows = xg[par]
        both = jnp.dot(rows, w13[par].reshape(-1, 2 * width), preferred_element_type=jnp.float32)
        hid = (jax.nn.silu(both[:, :width]) * both[:, width:]).astype(jnp.bfloat16)
        out = jnp.dot(hid, w2v[par].reshape(width, -1), preferred_element_type=jnp.float32)
        lane = lax.broadcasted_iota(jnp.int32, (cap, gb.shape[2]), 1)
        for m in range(2):
            gate = jnp.sum(jnp.where(lane == s, gb[m], 0.0), axis=1, keepdims=True)
            zst[par, m] = (out[m * cap:(m + 1) * cap] * gate).astype(jnp.bfloat16)

    def ready(s):
        for copy in weight_copies(wown, s % 2):
            copy.wait()
        row_in(s).wait()

    def fetch(s):
        for j in range(npos):
            @pl.when(s == 2 * j + 1)
            def _():
                ref = wall.at[expert(*ORDER[j], 1 - c)]
                pltpu.make_async_remote_copy(
                    src_ref=ref, dst_ref=ref, send_sem=d2d_send.at[0], recv_sem=d2d_recv.at[j],
                    device_id=partner, device_id_type=MESH).wait_recv()

        @pl.when(s > 0)
        def _():
            for copy in weight_copies(wall.at[step_expert(s)], s % 2):
                copy.start()
        row_in(s).start()

    def combine(base, groups, finish=None):
        items = 2 * groups

        def load(i):
            t = base + i % groups
            g = ((x + pick(t, GROUP_DX)) % RING) * 2 + (c + t) % 2
            return g, pltpu.make_async_copy(zh.at[g, i // groups], zc.at[i % 2], zl_sem.at[i % 2])

        load(0)[1].start()

        @pl.loop(0, items)
        def _(i):
            g, copy = load(i)
            copy.wait()

            @pl.when(i + 1 < items)
            def _():
                load(i + 1)[1].start()

            m = i // groups
            table = slotcol[m]
            lane = lax.broadcasted_iota(jnp.int32, table.shape, 1)
            lane_cap = lax.broadcasted_iota(jnp.int32, (tokens, cap), 1)
            parts = []
            for q in range(per_group):
                col = jnp.sum(jnp.where(lane == g * per_group + q, table, 0), axis=1, keepdims=True)
                parts.append((col == lane_cap).astype(jnp.bfloat16))
            sel = jnp.concatenate(parts, axis=1)
            part = jnp.dot(sel, zc[i % 2], preferred_element_type=jnp.float32)
            yacc[m] += part.astype(jnp.bfloat16).astype(jnp.float32)

            if finish is not None:
                @pl.when(i % groups == groups - 1)
                def _():
                    finish(m)

    steps = 2 * npos
    last = [2 * max(ORDER.index((dx, dy)) for dy in range(RING)) + 1 for dx in (0, 1, 3)]

    @pl.loop(0, steps + AHEAD)
    def _(v):
        s = v - AHEAD

        late = (s == last[0]) | (s == last[1]) | (s == last[2])

        @pl.when((v >= 2) & (v < steps + 2))
        def _():
            row_out(v - 2).wait()

        drained = (s < 2)
        for t in last:
            drained = drained | (s == t + 1) | (s == t + 2)

        @pl.when(jnp.logical_not(drained))
        def _():
            z_copy(s - 2).wait()

        def acts(phase):
            for unit in range(1, units + 1):
                if UNIT_STEP[unit][1] == phase:
                    @pl.when(v == UNIT_STEP[unit][0])
                    def _():
                        act(unit)

        acts(0)

        @pl.when((s >= -1) & (s + 1 < steps) & jnp.logical_not(late))
        def _():
            fetch(s + 1)

        @pl.when(v < AHEAD)
        def _():
            gather(v)

        @pl.when((v >= AHEAD) & (v < steps))
        def _():
            ready(s)
            ffn(s)
            gather(v)

        @pl.when(v >= steps)
        def _():
            ready(s)
            ffn(s)

        @pl.when(v < steps)
        def _():
            row_out(v).start()

        @pl.when(s >= 0)
        def _():
            z_copy(s).start()

        @pl.when(late)
        def _():
            z_copy(s - 1).wait()
            z_copy(s).wait()
            acts(1)
            combine(jnp.where(s == last[0], 0, jnp.where(s == last[1], 2, 4)), 2)
            acts(2)
            fetch(s + 1)

    z_copy(steps - 2).wait()
    z_copy(steps - 1).wait()

    def finish(m):
        @pl.loop(0, tokens // 128)
        def _(i):
            rows = pl.ds(pl.multiple_of(i * 128, 128), 128)
            xv[m, rows, :] = yacc[m, rows, :].astype(jnp.bfloat16)
        for n, dst in enumerate((y_first, y_second)):
            @pl.when(m == n)
            def _():
                pltpu.make_async_copy(xv.at[n], dst, y_sem.at[n]).start()

    combine(6, 2, finish)
    for m, dst in enumerate((y_first, y_second)):
        pltpu.make_async_copy(xv.at[m], dst, y_sem.at[m]).wait()

    for unit in range(units + 1):
        _, issued, complete = plan[unit]
        for link, slot, item, target in issued:
            quarter_copy(link, slot, item, target).wait_send()
        for pos in complete:
            d2d_copy(pos).wait_send()


def solution(mesh):
    n_grp = mesh.shape['grp']
    n_ing = mesh.shape['ing']
    assert n_grp == 2 * RING and n_ing == RING
    tok_spec = P(('dp', 'grp', 'ing'), None)
    w_spec = P(('grp', 'ing'), None, None)

    def body(x_first, ids_first, gates_first, x_second, ids_second, gates_second, w_one, w_three, w_two):
        tokens, hidden = x_first.shape
        top_k = ids_first.shape[1]
        experts = n_grp * n_ing
        limit_m = min(top_k, n_grp // 2)
        cap = limit_m * (-(-(tokens * (top_k // limit_m)) // experts))
        inner = w_one.shape[2]
        ids = jnp.stack([ids_first.T, ids_second.T])
        gates = jnp.stack([gates_first.T, gates_second.T])
        quarter = hidden // 4
        w2 = w_two[0].reshape(2, inner // 2, 2, hidden // 2).transpose(2, 0, 1, 3).reshape(4, inner // 2, hidden // 2)
        wown = jnp.stack([w_one[0].reshape(4, quarter, inner), w_three[0].reshape(4, quarter, inner), w2])
        bf, f32, i32 = jnp.bfloat16, jnp.float32, jnp.int32
        hbm = pl.BlockSpec(memory_space=pl.ANY)
        vmem = pl.BlockSpec(memory_space=pltpu.VMEM)
        dma = pltpu.SemaphoreType.DMA
        y_shape = jax.ShapeDtypeStruct((tokens, hidden), bf)
        outs = pl.pallas_call(
            functools.partial(kernel, cap),
            out_shape=(y_shape, y_shape,
                       jax.ShapeDtypeStruct((experts,) + wown.shape, bf),
                       jax.ShapeDtypeStruct((n_grp, 2, n_ing * cap, hidden), bf),
                       jax.ShapeDtypeStruct((experts, 2 * cap, hidden), bf)),
            in_specs=[hbm, hbm, vmem, vmem, hbm],
            out_specs=(hbm,) * 5,
            scratch_shapes=[
                pltpu.VMEM((2, tokens, hidden), bf),
                pltpu.VMEM((2, tokens, hidden), f32),
                pltpu.VMEM((2, 4, quarter, 2 * inner), bf),
                pltpu.VMEM((2, 2, quarter, hidden), bf),
                pltpu.VMEM((2, 2 * cap, hidden), bf),
                pltpu.VMEM((2, 2 * cap, hidden), bf),
                pltpu.VMEM((2, cap, 128), f32),
                pltpu.VMEM((2, 2, cap, hidden), bf),
                pltpu.VMEM((2, n_ing * cap, hidden), bf),
                pltpu.VMEM((2, experts, tokens), i32),
                pltpu.VMEM((2, experts, tokens), f32),
                pltpu.VMEM((2, tokens, 128), i32),
                dma((64,)), dma((60,)), dma((16,)), dma((16,)), dma((8,)), dma((2,)), dma((2,)), dma((2,)), dma((2,)), dma((2,)), dma((2,)),
            ],
            compiler_params=pltpu.CompilerParams(collective_id=0, has_side_effects=True, vmem_limit_bytes=67043328),
        )(x_first, x_second, ids, gates, wown)
        return outs[0], outs[1]

    return jax.shard_map(body, mesh=mesh, in_specs=(tok_spec,) * 6 + (w_spec,) * 3, out_specs=(tok_spec, tok_spec), check_vma=False)
```

```python
import functools

import jax
import jax.numpy as jnp
from jax import lax
from jax.experimental import pallas as pl
from jax.experimental.pallas import tpu as pltpu
from jax.sharding import PartitionSpec as P

MESH = pl.DeviceIdType.MESH
AHEAD = 24
RING = 4
ORDER = [(0, 0), (0, 1), (0, 3), (1, 0), (3, 0), (0, 2), (1, 1), (1, 3), (1, 2), (3, 1), (3, 3), (3, 2), (2, 0), (2, 1), (2, 3), (2, 2)]
GROUP_DX = [0, 0, 1, 1, 3, 3, 2, 2]
UNIT_STEP = {1: (5, 0), 2: (11, 0), 3: (18, 0), 4: (25, 0), 5: (28, 0), 6: (31, 0), 7: (35, 1), 8: (35, 2), 9: (39, 0), 10: (39, 0), 11: (41, 1), 12: (43, 0), 13: (47, 1), 14: (47, 2), 15: (52, 0)}


def link_sends():
    lists = []
    for d in (1, -1):
        kf, kg = (0, 2) if d > 0 else (1, 3)
        pair = (2, 3) if d > 0 else (3, 2)
        sends = [(0, 0, k) for k in (0, 1, 2, 3)] + [(0, b, k) for b in (1, -1, 2) for k in pair]
        sends += [(-d, 0, kf), (-d, 0, kg)] + [(-d, b, kg) for b in (1, -1, 2)]
        lists.append([(a % RING, b % RING, k) for a, b, k in sends])
    for d in (1, -1):
        kf, kg = (0, 2) if d > 0 else (1, 3)
        pair = (0, 1) if d > 0 else (1, 0)
        sends = [(0, 0, k) for k in (2, 3, 0, 1)] + [(0, -d, kg), (0, -d, kf)]
        for a in (1, -1, 2):
            sends += [(a, 0, k) for k in pair] + [(a, -d, kf)]
        lists.append([(a % RING, b % RING, k) for a, b, k in sends])
    return lists


STEP_OF_LINK = [(1, 0), (-1, 0), (0, 1), (0, -1)]


def make_plan():
    sends = link_sends()
    units = len(sends[0])
    shifted = lambda link, item: ((item[0] - STEP_OF_LINK[link][0]) % RING, (item[1] - STEP_OF_LINK[link][1]) % RING, item[2])
    have = {(0, 0, k) for k in range(4)}
    nxt = [0] * 4
    plan = {}
    done = set()
    for unit in range(units + 1):
        arrivals = [] if unit == 0 else [shifted(link, sends[link][unit - 1]) for link in range(4)]
        assert not have & set(arrivals)
        have |= set(arrivals)
        issued = []
        moved = True
        while moved:
            moved = False
            for link in range(4):
                if nxt[link] < units and sends[link][nxt[link]] in have:
                    issued.append((link, nxt[link], sends[link][nxt[link]], shifted(link, sends[link][nxt[link]])))
                    nxt[link] += 1
                    moved = True
        complete = [p for p in ORDER if p not in done and all((*p, k) in have for k in range(4))]
        done |= set(complete)
        plan[unit] = (arrivals, issued, complete)
    assert len(have) == 4 * RING * RING and nxt == [units] * 4
    return plan, units


def pick(index, values):
    out = jnp.int32(values[0])
    for i, v in enumerate(values[1:], 1):
        out = jnp.where(index == i, jnp.int32(v), out)
    return out


def kernel(cap, x_first, x_second, ids_first, ids_second, gates_first, gates_second, w_one, w_three, w_two, y_first, y_second, wall, zh, xh,
           xv, yacc, w13, w2v, xs, xg, gb, zst, zc, slotrow, gaterow, slotcol,
           recv_sem, send_sem, d2d_recv, d2d_send, w_sem, x_sem, xo_sem, xi_sem, z_sem, zl_sem, y_sem):
    grp, y = lax.axis_index('grp'), lax.axis_index('ing')
    x, c = grp // 2, grp % 2
    tokens = xv.shape[1]
    experts = slotrow.shape[1]
    per_group = RING
    width = wall.shape[4]
    quarter = wall.shape[3]
    plan, units = make_plan()
    npos = RING * RING

    def expert(dx, dy, core):
        return (((x + dx) % RING) * 2 + core) * per_group + (y + dy) % RING

    def neighbour(link):
        sx, sy = STEP_OF_LINK[link]
        return {'grp': ((x + sx) % RING) * 2 + c, 'ing': (y + sy) % RING}

    partner = {'grp': x * 2 + (1 - c), 'ing': y}

    barrier = pltpu.get_barrier_semaphore()
    for dev in [neighbour(link) for link in range(4)] + [partner]:
        pl.semaphore_signal(barrier, inc=1, device_id=dev, device_id_type=MESH)
    pl.semaphore_wait(barrier, 5)

    def own_piece(part, k):
        if part < 2:
            return (w_one, w_three)[part].at[0, pl.ds(k * quarter, quarter), :]
        return w_two.at[0, pl.ds((k % 2) * quarter, quarter), pl.ds((k // 2) * width, width)]

    def quarter_copies(link, slot, item, target):
        dx, dy, k = item
        dst = wall.at[expert(dx, dy, c), :, k]
        own = (dx, dy) == (0, 0)
        pairs = [(own_piece(part, k), dst.at[part]) for part in range(3)] if own else [(dst, dst)]
        return [pltpu.make_async_remote_copy(
            src_ref=src, dst_ref=to, send_sem=send_sem.at[link * units + slot],
            recv_sem=recv_sem.at[(target[0] * RING + target[1]) * 4 + k], device_id=neighbour(link), device_id_type=MESH)
            for src, to in pairs]

    def d2d_copies(pos):
        j = ORDER.index(pos)
        dst = wall.at[expert(*pos, c)]
        pairs = [(own_piece(part, k), dst.at[part, k]) for part in range(3) for k in range(4)] if j == 0 else [(dst, dst)]
        return [pltpu.make_async_remote_copy(
            src_ref=src, dst_ref=to, send_sem=d2d_send.at[j], recv_sem=d2d_recv.at[j],
            device_id=partner, device_id_type=MESH) for src, to in pairs]

    def sent(ref, sem):
        pltpu.make_async_remote_copy(
            src_ref=ref, dst_ref=ref, send_sem=sem, recv_sem=recv_sem.at[0], device_id=partner, device_id_type=MESH).wait_send()

    def act(unit):
        arrivals, issued, complete = plan[unit]
        for dx, dy, k in arrivals:
            ref = wall.at[expert(dx, dy, c), :, k]
            pltpu.make_async_remote_copy(
                src_ref=ref, dst_ref=ref, send_sem=send_sem.at[0], recv_sem=recv_sem.at[(dx * RING + dy) * 4 + k],
                device_id=partner, device_id_type=MESH).wait_recv()
        for link, slot, item, target in issued:
            for copy in quarter_copies(link, slot, item, target):
                copy.start()
        for pos in complete:
            for copy in d2d_copies(pos):
                copy.start()

    act(0)
    x_copies = [pltpu.make_async_copy(src, xv.at[m], x_sem.at[m]) for m, src in enumerate((x_first, x_second))]
    for copy in x_copies:
        copy.start()

    def weight_copies(src, par):
        for half in range(2):
            yield pltpu.make_async_copy(src.at[half], w13.at[par, :, :, pl.ds(half * width, width)], w_sem.at[par * 4 + half])
        for half in range(2):
            yield pltpu.make_async_copy(src.at[2, pl.ds(2 * half, 2)], w2v.at[par, :, :, pl.ds(half * width, width)], w_sem.at[par * 4 + 2 + half])

    for k in range(4):
        for part in range(2):
            pltpu.make_async_copy(own_piece(part, k), w13.at[0, k, :, pl.ds(part * width, width)], w_sem.at[part]).start()
        pltpu.make_async_copy(own_piece(2, k), w2v.at[0, k % 2, :, pl.ds((k // 2) * width, width)], w_sem.at[2 + k // 2]).start()

    lane_block = 128
    upper = (lax.broadcasted_iota(jnp.int32, (lane_block, lane_block), 0)
             <= lax.broadcasted_iota(jnp.int32, (lane_block, lane_block), 1)).astype(jnp.bfloat16)
    for m in range(2):
        e_iota = lax.broadcasted_iota(jnp.int32, (experts, lane_block), 0)
        carry = jnp.zeros((experts, 1), jnp.float32)
        for b in range(tokens // lane_block):
            cols = pl.ds(b * lane_block, lane_block)
            mem = jnp.zeros((experts, lane_block), jnp.float32)
            gat = jnp.zeros((experts, lane_block), jnp.float32)
            for k in range(ids_first.shape[0]):
                hit = (ids_first, ids_second)[m][k:k + 1, cols] == e_iota
                mem = jnp.where(hit, 1.0, mem)
                gat = jnp.where(hit, (gates_first, gates_second)[m][k:k + 1, cols], gat)
            total = jnp.dot(mem.astype(jnp.bfloat16), upper, preferred_element_type=jnp.float32) + carry
            carry = carry + jnp.sum(mem, axis=1, keepdims=True)
            slot = jnp.where(mem > 0.0, total - 1.0, -1.0)
            slotrow[m, :, cols] = slot.astype(jnp.int32)
            gaterow[m, :, cols] = gat
            full = jnp.concatenate([slot, jnp.full((lane_block - experts, lane_block), -1.0, jnp.float32)], axis=0)
            slotcol[m, cols, :] = full.T.astype(jnp.int32)

    gb[...] = jnp.zeros_like(gb)
    for m in range(2):
        @pl.loop(0, tokens // 128)
        def _(i):
            yacc[m, pl.ds(i * 128, 128), :] = jnp.zeros((128, yacc.shape[2]), jnp.float32)

    for copy in x_copies:
        copy.wait()

    def step_expert(s):
        j = s // 2
        core = (c + s) % 2
        return expert(pick(j, [p[0] for p in ORDER]), pick(j, [p[1] for p in ORDER]), core)

    def gather(s):
        e = step_expert(s)
        lane = lax.broadcasted_iota(jnp.int32, (cap, gb.shape[2]), 1)
        for m in range(2):
            mask = slotrow[m, pl.ds(e, 1), :] == lax.broadcasted_iota(jnp.int32, (cap, tokens), 0)
            gate = jnp.sum(jnp.where(mask, gaterow[m, pl.ds(e, 1), :], 0.0), axis=1, keepdims=True)
            gb[m] = jnp.where(lane == s, gate, gb[m])
            xs[s % 2, m * cap:(m + 1) * cap, :] = jnp.dot(
                mask.astype(jnp.bfloat16), xv[m], preferred_element_type=jnp.float32).astype(jnp.bfloat16)

    def row_out(s):
        return pltpu.make_async_copy(xs.at[s % 2], xh.at[s], xo_sem.at[s % 2])

    def row_in(s):
        return pltpu.make_async_copy(xh.at[s], xg.at[s % 2], xi_sem.at[s % 2])

    def z_copy(s):
        e = step_expert(s)
        return pltpu.make_async_copy(zst.at[s % 2], zh.at[e // per_group, :, pl.ds((e % per_group) * cap, cap), :], z_sem.at[s % 2])

    def ffn(s):
        par = s % 2
        rows = xg[par]
        both = jnp.dot(rows, w13[par].reshape(-1, 2 * width), preferred_element_type=jnp.float32)
        hid = (jax.nn.silu(both[:, :width]) * both[:, width:]).astype(jnp.bfloat16)
        out = jnp.dot(hid, w2v[par].reshape(width, -1), preferred_element_type=jnp.float32)
        lane = lax.broadcasted_iota(jnp.int32, (cap, gb.shape[2]), 1)
        for m in range(2):
            gate = jnp.sum(jnp.where(lane == s, gb[m], 0.0), axis=1, keepdims=True)
            zst[par, m] = (out[m * cap:(m + 1) * cap] * gate).astype(jnp.bfloat16)

    def ready(s):
        for copy in weight_copies(wall.at[0], s % 2):
            copy.wait()
        row_in(s).wait()

    def fetch(s):
        for j in range(npos):
            @pl.when(s == 2 * j + 1)
            def _():
                ref = wall.at[expert(*ORDER[j], 1 - c)]
                pltpu.make_async_remote_copy(
                    src_ref=ref, dst_ref=ref, send_sem=d2d_send.at[0], recv_sem=d2d_recv.at[j],
                    device_id=partner, device_id_type=MESH).wait_recv()

        @pl.when(s > 0)
        def _():
            for copy in weight_copies(wall.at[step_expert(s)], s % 2):
                copy.start()
        row_in(s).start()

    def combine(base, groups, step, near_end=None, finish=None):
        items = 2 * groups

        def load(i):
            t = base + i % groups
            g = ((x + pick(t, GROUP_DX)) % RING) * 2 + (c + t) % 2
            return g, pltpu.make_async_copy(zh.at[g, i // groups], zc.at[i % 2], zl_sem.at[i % 2])

        load(0)[1].start()

        @pl.loop(0, items)
        def _(i):
            g, copy = load(i)
            copy.wait()

            @pl.when(i == 0)
            def _():
                z_copy(step).wait()

            @pl.when(i + 1 < items)
            def _():
                load(i + 1)[1].start()

            if near_end is not None:
                @pl.when(i == items - 1)
                def _():
                    near_end()

            m = i // groups
            table = slotcol[m]
            lane = lax.broadcasted_iota(jnp.int32, table.shape, 1)
            lane_cap = lax.broadcasted_iota(jnp.int32, (tokens, cap), 1)
            parts = []
            for q in range(per_group):
                col = jnp.sum(jnp.where(lane == g * per_group + q, table, 0), axis=1, keepdims=True)
                parts.append((col == lane_cap).astype(jnp.bfloat16))
            sel = jnp.concatenate(parts, axis=1)
            part = jnp.dot(sel, zc[i % 2], preferred_element_type=jnp.float32)
            yacc[m] += part.astype(jnp.bfloat16).astype(jnp.float32)

            if finish is not None:
                @pl.when(i % groups == groups - 1)
                def _():
                    finish(m)

    steps = 2 * npos
    last = [2 * max(ORDER.index((dx, dy)) for dy in range(RING)) + 1 for dx in (0, 1, 3)]

    @pl.loop(0, steps + AHEAD)
    def _(v):
        s = v - AHEAD

        late = (s == last[0]) | (s == last[1]) | (s == last[2])

        @pl.when((v >= 2) & (v < steps + 2))
        def _():
            row_out(v - 2).wait()

        drained = (s < 2)
        for t in last:
            drained = drained | (s == t + 1) | (s == t + 2)

        @pl.when(jnp.logical_not(drained))
        def _():
            z_copy(s - 2).wait()

        def acts(phase):
            for unit in range(1, units + 1):
                if UNIT_STEP[unit][1] == phase:
                    @pl.when(v == UNIT_STEP[unit][0])
                    def _():
                        act(unit)

        acts(0)

        @pl.when((s >= -1) & (s + 1 < steps) & jnp.logical_not(late))
        def _():
            fetch(s + 1)

        @pl.when(v < AHEAD)
        def _():
            gather(v)

        @pl.when((v >= AHEAD) & (v < steps))
        def _():
            ready(s)
            ffn(s)
            gather(v)

        @pl.when(v >= steps)
        def _():
            ready(s)
            ffn(s)

        @pl.when(v < steps)
        def _():
            row_out(v).start()

        @pl.when(s >= 0)
        def _():
            z_copy(s).start()

        @pl.when(late)
        def _():
            z_copy(s - 1).wait()
            acts(1)

            def near_end():
                acts(2)
                fetch(s + 1)

            combine(jnp.where(s == last[0], 0, jnp.where(s == last[1], 2, 4)), 2, s, near_end)

    z_copy(steps - 2).wait()

    def finish(m):
        @pl.loop(0, tokens // 128)
        def _(i):
            rows = pl.ds(pl.multiple_of(i * 128, 128), 128)
            xv[m, rows, :] = yacc[m, rows, :].astype(jnp.bfloat16)
        for n, dst in enumerate((y_first, y_second)):
            @pl.when(m == n)
            def _():
                pltpu.make_async_copy(xv.at[n], dst, y_sem.at[n]).start()

    combine(6, 2, steps - 1, None, finish)
    for m, dst in enumerate((y_first, y_second)):
        pltpu.make_async_copy(xv.at[m], dst, y_sem.at[m]).wait()

    for unit in range(units + 1):
        _, issued, complete = plan[unit]
        for link, slot, item, target in issued:
            sent(wall.at[expert(item[0], item[1], c), :, item[2]], send_sem.at[link * units + slot])
        for pos in complete:
            sent(wall.at[expert(*pos, c)], d2d_send.at[ORDER.index(pos)])


def solution(mesh):
    n_grp = mesh.shape['grp']
    n_ing = mesh.shape['ing']
    assert n_grp == 2 * RING and n_ing == RING
    tok_spec = P(('dp', 'grp', 'ing'), None)
    w_spec = P(('grp', 'ing'), None, None)

    def body(x_first, ids_first, gates_first, x_second, ids_second, gates_second, w_one, w_three, w_two):
        tokens, hidden = x_first.shape
        top_k = ids_first.shape[1]
        experts = n_grp * n_ing
        limit_m = min(top_k, n_grp // 2)
        cap = limit_m * (-(-(tokens * (top_k // limit_m)) // experts))
        inner = w_one.shape[2]
        quarter = hidden // 4
        wall_shape = (experts, 3, 4, quarter, inner)
        bf, f32, i32 = jnp.bfloat16, jnp.float32, jnp.int32
        hbm = pl.BlockSpec(memory_space=pl.ANY)
        vmem = pl.BlockSpec(memory_space=pltpu.VMEM)
        dma = pltpu.SemaphoreType.DMA
        y_shape = jax.ShapeDtypeStruct((tokens, hidden), bf)
        outs = pl.pallas_call(
            functools.partial(kernel, cap),
            out_shape=(y_shape, y_shape,
                       jax.ShapeDtypeStruct(wall_shape, bf),
                       jax.ShapeDtypeStruct((n_grp, 2, n_ing * cap, hidden), bf),
                       jax.ShapeDtypeStruct((experts, 2 * cap, hidden), bf)),
            in_specs=[hbm] * 2 + [vmem] * 4 + [hbm] * 3,
            out_specs=(hbm,) * 5,
            scratch_shapes=[
                pltpu.VMEM((2, tokens, hidden), bf),
                pltpu.VMEM((2, tokens, hidden), f32),
                pltpu.VMEM((2, 4, quarter, 2 * inner), bf),
                pltpu.VMEM((2, 2, quarter, hidden), bf),
                pltpu.VMEM((2, 2 * cap, hidden), bf),
                pltpu.VMEM((2, 2 * cap, hidden), bf),
                pltpu.VMEM((2, cap, 128), f32),
                pltpu.VMEM((2, 2, cap, hidden), bf),
                pltpu.VMEM((2, n_ing * cap, hidden), bf),
                pltpu.VMEM((2, experts, tokens), i32),
                pltpu.VMEM((2, experts, tokens), f32),
                pltpu.VMEM((2, tokens, 128), i32),
                dma((64,)), dma((60,)), dma((16,)), dma((16,)), dma((8,)), dma((2,)), dma((2,)), dma((2,)), dma((2,)), dma((2,)), dma((2,)),
            ],
            compiler_params=pltpu.CompilerParams(collective_id=0, has_side_effects=True, vmem_limit_bytes=67043328),
        )(x_first, x_second, ids_first.T, ids_second.T, gates_first.T, gates_second.T, w_one, w_three, w_two)
        return outs[0], outs[1]

    return jax.shard_map(body, mesh=mesh, in_specs=(tok_spec,) * 6 + (w_spec,) * 3, out_specs=(tok_spec, tok_spec), check_vma=False)
```

```python
import functools

import jax
import jax.numpy as jnp
from jax import lax
from jax.experimental import pallas as pl
from jax.experimental.pallas import tpu as pltpu
from jax.sharding import PartitionSpec as P

MESH = pl.DeviceIdType.MESH
AHEAD = 24
RING = 4
ORDER = [(0, 0), (0, 1), (0, 3), (1, 0), (3, 0), (0, 2), (1, 1), (1, 3), (1, 2), (3, 1), (3, 3), (3, 2), (2, 0), (2, 1), (2, 3), (2, 2)]
GROUP_DX = [0, 0, 1, 1, 3, 3, 2, 2]
UNIT_STEP = {1: (5, 0), 2: (11, 0), 3: (18, 0), 4: (25, 0), 5: (28, 0), 6: (31, 0), 7: (35, 1), 8: (35, 2), 9: (39, 0), 10: (39, 0), 11: (41, 1), 12: (43, 0), 13: (47, 1), 14: (47, 2), 15: (52, 0)}


def link_sends():
    lists = []
    for d in (1, -1):
        kf, kg = (0, 2) if d > 0 else (1, 3)
        pair = (2, 3) if d > 0 else (3, 2)
        sends = [(0, 0, k) for k in (0, 1, 2, 3)] + [(0, b, k) for b in (1, -1, 2) for k in pair]
        sends += [(-d, 0, kf), (-d, 0, kg)] + [(-d, b, kg) for b in (1, -1, 2)]
        lists.append([(a % RING, b % RING, k) for a, b, k in sends])
    for d in (1, -1):
        kf, kg = (0, 2) if d > 0 else (1, 3)
        pair = (0, 1) if d > 0 else (1, 0)
        sends = [(0, 0, k) for k in (2, 3, 0, 1)] + [(0, -d, kg), (0, -d, kf)]
        for a in (1, -1, 2):
            sends += [(a, 0, k) for k in pair] + [(a, -d, kf)]
        lists.append([(a % RING, b % RING, k) for a, b, k in sends])
    return lists


STEP_OF_LINK = [(1, 0), (-1, 0), (0, 1), (0, -1)]


def make_plan():
    sends = link_sends()
    units = len(sends[0])
    shifted = lambda link, item: ((item[0] - STEP_OF_LINK[link][0]) % RING, (item[1] - STEP_OF_LINK[link][1]) % RING, item[2])
    have = {(0, 0, k) for k in range(4)}
    nxt = [0] * 4
    plan = {}
    done = set()
    for unit in range(units + 1):
        arrivals = [] if unit == 0 else [shifted(link, sends[link][unit - 1]) for link in range(4)]
        assert not have & set(arrivals)
        have |= set(arrivals)
        issued = []
        moved = True
        while moved:
            moved = False
            for link in range(4):
                if nxt[link] < units and sends[link][nxt[link]] in have:
                    issued.append((link, nxt[link], sends[link][nxt[link]], shifted(link, sends[link][nxt[link]])))
                    nxt[link] += 1
                    moved = True
        complete = [p for p in ORDER if p not in done and all((*p, k) in have for k in range(4))]
        done |= set(complete)
        plan[unit] = (arrivals, issued, complete)
    assert len(have) == 4 * RING * RING and nxt == [units] * 4
    return plan, units


def pick(index, values):
    out = jnp.int32(values[0])
    for i, v in enumerate(values[1:], 1):
        out = jnp.where(index == i, jnp.int32(v), out)
    return out


def kernel(cap, x_first, x_second, ids_first, ids_second, gates_first, gates_second, w_one, w_three, w_two, y_first, y_second, wall, zh, xh,
           xv, yacc, w13, w2v, xs, xg, gb, zst, zc, slotrow, gaterow, slotcol,
           recv_sem, send_sem, d2d_recv, d2d_send, w_sem, x_sem, xo_sem, xi_sem, z_sem, zl_sem, y_sem):
    grp, y = lax.axis_index('grp'), lax.axis_index('ing')
    x, c = grp // 2, grp % 2
    tokens = xv.shape[1]
    experts = slotrow.shape[1]
    per_group = RING
    width = wall.shape[4]
    quarter = wall.shape[3]
    plan, units = make_plan()
    npos = RING * RING

    def expert(dx, dy, core):
        return (((x + dx) % RING) * 2 + core) * per_group + (y + dy) % RING

    def neighbour(link):
        sx, sy = STEP_OF_LINK[link]
        return {'grp': ((x + sx) % RING) * 2 + c, 'ing': (y + sy) % RING}

    partner = {'grp': x * 2 + (1 - c), 'ing': y}

    barrier = pltpu.get_barrier_semaphore()
    for dev in [neighbour(link) for link in range(4)] + [partner]:
        pl.semaphore_signal(barrier, inc=1, device_id=dev, device_id_type=MESH)
    pl.semaphore_wait(barrier, 5)

    def own_piece(part, k):
        if part < 2:
            return (w_one, w_three)[part].at[0, pl.ds(k * quarter, quarter), :]
        return w_two.at[0, pl.ds((k % 2) * quarter, quarter), pl.ds((k // 2) * width, width)]

    def quarter_copies(link, slot, item, target):
        dx, dy, k = item
        dst = wall.at[expert(dx, dy, c), :, k]
        own = (dx, dy) == (0, 0)
        pairs = [(own_piece(part, k), dst.at[part]) for part in range(3)] if own else [(dst, dst)]
        return [pltpu.make_async_remote_copy(
            src_ref=src, dst_ref=to, send_sem=send_sem.at[link * units + slot],
            recv_sem=recv_sem.at[(target[0] * RING + target[1]) * 4 + k], device_id=neighbour(link), device_id_type=MESH)
            for src, to in pairs]

    def d2d_copies(dx, dy, k):
        j = ORDER.index((dx, dy))
        dst = wall.at[expert(dx, dy, c), :, k]
        pairs = [(own_piece(part, k), dst.at[part]) for part in range(3)] if j == 0 else [(dst, dst)]
        return [pltpu.make_async_remote_copy(
            src_ref=src, dst_ref=to, send_sem=d2d_send.at[j], recv_sem=d2d_recv.at[j],
            device_id=partner, device_id_type=MESH) for src, to in pairs]

    def sent(ref, sem):
        pltpu.make_async_remote_copy(
            src_ref=ref, dst_ref=ref, send_sem=sem, recv_sem=recv_sem.at[0], device_id=partner, device_id_type=MESH).wait_send()

    def act(unit):
        arrivals, issued, _ = plan[unit]
        for dx, dy, k in arrivals:
            ref = wall.at[expert(dx, dy, c), :, k]
            pltpu.make_async_remote_copy(
                src_ref=ref, dst_ref=ref, send_sem=send_sem.at[0], recv_sem=recv_sem.at[(dx * RING + dy) * 4 + k],
                device_id=partner, device_id_type=MESH).wait_recv()
        for link, slot, item, target in issued:
            for copy in quarter_copies(link, slot, item, target):
                copy.start()
        for dx, dy, k in arrivals or [(0, 0, k) for k in range(4)]:
            for copy in d2d_copies(dx, dy, k):
                copy.start()

    act(0)
    x_copies = [pltpu.make_async_copy(src, xv.at[m], x_sem.at[m]) for m, src in enumerate((x_first, x_second))]
    for copy in x_copies:
        copy.start()

    def weight_copies(src, par):
        for half in range(2):
            yield pltpu.make_async_copy(src.at[half], w13.at[par, :, :, pl.ds(half * width, width)], w_sem.at[par * 4 + half])
        for half in range(2):
            yield pltpu.make_async_copy(src.at[2, pl.ds(2 * half, 2)], w2v.at[par, :, :, pl.ds(half * width, width)], w_sem.at[par * 4 + 2 + half])

    for k in range(4):
        for part in range(2):
            pltpu.make_async_copy(own_piece(part, k), w13.at[0, k, :, pl.ds(part * width, width)], w_sem.at[part]).start()
        pltpu.make_async_copy(own_piece(2, k), w2v.at[0, k % 2, :, pl.ds((k // 2) * width, width)], w_sem.at[2 + k // 2]).start()

    lane_block = 128
    upper = (lax.broadcasted_iota(jnp.int32, (lane_block, lane_block), 0)
             <= lax.broadcasted_iota(jnp.int32, (lane_block, lane_block), 1)).astype(jnp.bfloat16)
    for m in range(2):
        e_iota = lax.broadcasted_iota(jnp.int32, (experts, lane_block), 0)
        carry = jnp.zeros((experts, 1), jnp.float32)
        for b in range(tokens // lane_block):
            cols = pl.ds(b * lane_block, lane_block)
            mem = jnp.zeros((experts, lane_block), jnp.float32)
            gat = jnp.zeros((experts, lane_block), jnp.float32)
            for k in range(ids_first.shape[0]):
                hit = (ids_first, ids_second)[m][k:k + 1, cols] == e_iota
                mem = jnp.where(hit, 1.0, mem)
                gat = jnp.where(hit, (gates_first, gates_second)[m][k:k + 1, cols], gat)
            total = jnp.dot(mem.astype(jnp.bfloat16), upper, preferred_element_type=jnp.float32) + carry
            carry = carry + jnp.sum(mem, axis=1, keepdims=True)
            slot = jnp.where(mem > 0.0, total - 1.0, -1.0)
            slotrow[m, :, cols] = slot.astype(jnp.int32)
            gaterow[m, :, cols] = gat
            full = jnp.concatenate([slot, jnp.full((lane_block - experts, lane_block), -1.0, jnp.float32)], axis=0)
            slotcol[m, cols, :] = full.T

    gb[...] = jnp.zeros_like(gb)
    for m in range(2):
        @pl.loop(0, tokens // 128)
        def _(i):
            yacc[m, pl.ds(i * 128, 128), :] = jnp.zeros((128, yacc.shape[2]), jnp.float32)

    for copy in x_copies:
        copy.wait()

    def step_expert(s):
        j = s // 2
        core = (c + s) % 2
        return expert(pick(j, [p[0] for p in ORDER]), pick(j, [p[1] for p in ORDER]), core)

    def gather(s):
        e = step_expert(s)
        lane = lax.broadcasted_iota(jnp.int32, (cap, gb.shape[2]), 1)
        for m in range(2):
            mask = slotrow[m, pl.ds(e, 1), :] == lax.broadcasted_iota(jnp.int32, (cap, tokens), 0)
            gate = jnp.sum(jnp.where(mask, gaterow[m, pl.ds(e, 1), :], 0.0), axis=1, keepdims=True)
            gb[m] = jnp.where(lane == s, gate, gb[m])
            xs[s % 2, m * cap:(m + 1) * cap, :] = jnp.dot(
                mask.astype(jnp.bfloat16), xv[m], preferred_element_type=jnp.float32).astype(jnp.bfloat16)

    def row_out(s):
        return pltpu.make_async_copy(xs.at[s % 2], xh.at[s], xo_sem.at[s % 2])

    def row_in(s):
        return pltpu.make_async_copy(xh.at[s], xg.at[s % 2], xi_sem.at[s % 2])

    def z_copy(s):
        e = step_expert(s)
        return pltpu.make_async_copy(zst.at[s % 2], zh.at[e // per_group, :, pl.ds((e % per_group) * cap, cap), :], z_sem.at[s % 2])

    def ffn(s):
        par = s % 2
        rows = xg[par]
        both = jnp.dot(rows, w13[par].reshape(-1, 2 * width), preferred_element_type=jnp.float32)
        hid = (jax.nn.silu(both[:, :width]) * both[:, width:]).astype(jnp.bfloat16)
        out = jnp.dot(hid, w2v[par].reshape(width, -1), preferred_element_type=jnp.float32)
        lane = lax.broadcasted_iota(jnp.int32, (cap, gb.shape[2]), 1)
        for m in range(2):
            gate = jnp.sum(jnp.where(lane == s, gb[m], 0.0), axis=1, keepdims=True)
            zst[par, m] = (out[m * cap:(m + 1) * cap] * gate).astype(jnp.bfloat16)

    def ready(s):
        for copy in weight_copies(wall.at[0], s % 2):
            copy.wait()
        row_in(s).wait()

    def fetch(s):
        for j in range(npos):
            @pl.when(s == 2 * j + 1)
            def _():
                ref = wall.at[expert(*ORDER[j], 1 - c)]
                pltpu.make_async_remote_copy(
                    src_ref=ref, dst_ref=ref, send_sem=d2d_send.at[0], recv_sem=d2d_recv.at[j],
                    device_id=partner, device_id_type=MESH).wait_recv()

        @pl.when(s > 0)
        def _():
            for copy in weight_copies(wall.at[step_expert(s)], s % 2):
                copy.start()
        row_in(s).start()

    def combine(base, groups, step, near_end=None, finish=None):
        items = 2 * groups

        def load(i):
            t = base + i % groups
            g = ((x + pick(t, GROUP_DX)) % RING) * 2 + (c + t) % 2
            return g, pltpu.make_async_copy(zh.at[g, i // groups], zc.at[i % 2], zl_sem.at[i % 2])

        load(0)[1].start()

        @pl.loop(0, items)
        def _(i):
            g, copy = load(i)
            copy.wait()

            @pl.when(i == 0)
            def _():
                z_copy(step).wait()

            @pl.when(i + 1 < items)
            def _():
                load(i + 1)[1].start()

            if near_end is not None:
                @pl.when(i == items - 1)
                def _():
                    near_end()

            m = i // groups
            table = slotcol[m]
            lane = lax.broadcasted_iota(jnp.int32, table.shape, 1)
            lane_cap = lax.broadcasted_iota(jnp.int32, (tokens, cap), 1).astype(jnp.float32)
            parts = []
            for q in range(per_group):
                col = jnp.sum(jnp.where(lane == g * per_group + q, table, 0.0), axis=1, keepdims=True)
                parts.append((col == lane_cap).astype(jnp.bfloat16))
            sel = jnp.concatenate(parts, axis=1)
            part = jnp.dot(sel, zc[i % 2], preferred_element_type=jnp.float32)
            yacc[m] += part.astype(jnp.bfloat16).astype(jnp.float32)

            if finish is not None:
                @pl.when(i % groups == groups - 1)
                def _():
                    finish(m)

    steps = 2 * npos
    last = [2 * max(ORDER.index((dx, dy)) for dy in range(RING)) + 1 for dx in (0, 1, 3)]

    @pl.loop(0, steps + AHEAD)
    def _(v):
        s = v - AHEAD

        late = (s == last[0]) | (s == last[1]) | (s == last[2])

        @pl.when((v >= 2) & (v < steps + 2))
        def _():
            row_out(v - 2).wait()

        drained = (s < 2)
        for t in last:
            drained = drained | (s == t + 1) | (s == t + 2)

        @pl.when(jnp.logical_not(drained))
        def _():
            z_copy(s - 2).wait()

        def acts(phase):
            for unit in range(1, units + 1):
                if UNIT_STEP[unit][1] == phase:
                    @pl.when(v == UNIT_STEP[unit][0])
                    def _():
                        act(unit)

        acts(0)

        @pl.when((s >= -1) & (s + 1 < steps) & jnp.logical_not(late))
        def _():
            fetch(s + 1)

        @pl.when(v < AHEAD)
        def _():
            gather(v)

        @pl.when((v >= AHEAD) & (v < steps))
        def _():
            ready(s)
            ffn(s)
            gather(v)

        @pl.when(v >= steps)
        def _():
            ready(s)
            ffn(s)

        @pl.when(v < steps)
        def _():
            row_out(v).start()

        @pl.when(s >= 0)
        def _():
            z_copy(s).start()

        @pl.when(late)
        def _():
            z_copy(s - 1).wait()
            acts(1)

            def near_end():
                acts(2)
                fetch(s + 1)

            combine(jnp.where(s == last[0], 0, jnp.where(s == last[1], 2, 4)), 2, s, near_end)

    z_copy(steps - 2).wait()

    def finish(m):
        @pl.loop(0, tokens // 128)
        def _(i):
            rows = pl.ds(pl.multiple_of(i * 128, 128), 128)
            xv[m, rows, :] = yacc[m, rows, :].astype(jnp.bfloat16)
        for n, dst in enumerate((y_first, y_second)):
            @pl.when(m == n)
            def _():
                pltpu.make_async_copy(xv.at[n], dst, y_sem.at[n]).start()

    combine(6, 2, steps - 1, None, finish)
    for m, dst in enumerate((y_first, y_second)):
        pltpu.make_async_copy(xv.at[m], dst, y_sem.at[m]).wait()

    for unit in range(units + 1):
        _, issued, complete = plan[unit]
        for link, slot, item, target in issued:
            sent(wall.at[expert(item[0], item[1], c), :, item[2]], send_sem.at[link * units + slot])
        for pos in complete:
            sent(wall.at[expert(*pos, c)], d2d_send.at[ORDER.index(pos)])


def solution(mesh):
    n_grp = mesh.shape['grp']
    n_ing = mesh.shape['ing']
    assert n_grp == 2 * RING and n_ing == RING
    tok_spec = P(('dp', 'grp', 'ing'), None)
    w_spec = P(('grp', 'ing'), None, None)

    def body(x_first, ids_first, gates_first, x_second, ids_second, gates_second, w_one, w_three, w_two):
        tokens, hidden = x_first.shape
        top_k = ids_first.shape[1]
        experts = n_grp * n_ing
        limit_m = min(top_k, n_grp // 2)
        cap = limit_m * (-(-(tokens * (top_k // limit_m)) // experts))
        inner = w_one.shape[2]
        quarter = hidden // 4
        wall_shape = (experts, 3, 4, quarter, inner)
        bf, f32, i32 = jnp.bfloat16, jnp.float32, jnp.int32
        hbm = pl.BlockSpec(memory_space=pl.ANY)
        vmem = pl.BlockSpec(memory_space=pltpu.VMEM)
        dma = pltpu.SemaphoreType.DMA
        y_shape = jax.ShapeDtypeStruct((tokens, hidden), bf)
        outs = pl.pallas_call(
            functools.partial(kernel, cap),
            out_shape=(y_shape, y_shape,
                       jax.ShapeDtypeStruct(wall_shape, bf),
                       jax.ShapeDtypeStruct((n_grp, 2, n_ing * cap, hidden), bf),
                       jax.ShapeDtypeStruct((experts, 2 * cap, hidden), bf)),
            in_specs=[hbm] * 2 + [vmem] * 4 + [hbm] * 3,
            out_specs=(hbm,) * 5,
            scratch_shapes=[
                pltpu.VMEM((2, tokens, hidden), bf),
                pltpu.VMEM((2, tokens, hidden), f32),
                pltpu.VMEM((2, 4, quarter, 2 * inner), bf),
                pltpu.VMEM((2, 2, quarter, hidden), bf),
                pltpu.VMEM((2, 2 * cap, hidden), bf),
                pltpu.VMEM((2, 2 * cap, hidden), bf),
                pltpu.VMEM((2, cap, 128), f32),
                pltpu.VMEM((2, 2, cap, hidden), bf),
                pltpu.VMEM((2, n_ing * cap, hidden), bf),
                pltpu.VMEM((2, experts, tokens), i32),
                pltpu.VMEM((2, experts, tokens), f32),
                pltpu.VMEM((2, tokens, 128), f32),
                dma((64,)), dma((60,)), dma((16,)), dma((16,)), dma((8,)), dma((2,)), dma((2,)), dma((2,)), dma((2,)), dma((2,)), dma((2,)),
            ],
            compiler_params=pltpu.CompilerParams(collective_id=0, has_side_effects=True, vmem_limit_bytes=67043328),
        )(x_first, x_second, ids_first.T, ids_second.T, gates_first.T, gates_second.T, w_one, w_three, w_two)
        return outs[0], outs[1]

    return jax.shard_map(body, mesh=mesh, in_specs=(tok_spec,) * 6 + (w_spec,) * 3, out_specs=(tok_spec, tok_spec), check_vma=False)
```
